32 devices in a mesh: mom: 8 (over y, x, core), en: 4 (over z).
Axes of the slice: x: 2, y: 2, z: 4, core: 2. Of those that a mesh axis runs over, the one named last changes fastest.
Arguments:
- green: bfloat16 [2, 8, 16, 2, 128, 128], P(None, 'mom', 'en'), may hold values from -0.5 to 0.5
- bare: bfloat16 [2, 8, 16, 2, 128, 128], P(None, 'mom', 'en'), may hold values from -0.5 to 0.5
- coupling: bfloat16 [4, 128, 128], replicated, may hold values from -0.25 to 0.25
- occupation: float32 [4], replicated, may hold values from 0.2 to 2
- mode_shift: int32 [4], replicated, may hold values from -1 to 1, as said below
- mode_offset: int32 [4], replicated, may hold values from 1 to 4, as said below
- mode_block: int32 [2, 4], replicated, may hold values from 0 to 1
Outputs:
- updated: bfloat16 [2, 8, 16, 2, 128, 128], P(None, 'mom', 'en')
The draws below stay inside these ranges and needn't reach their ends.
Inputs may be any that keep to these rules, and one draw needn't show every extreme that they name: `mode_shift`: each of -1, 0 and 1 is the shift of some mode. `mode_offset`: every offset from 1 to 4 is some mode's.
All inputs are finite; a program needn't handle non-finite values.
Results may differ from the reference program's by a relative error of at most 0.02.
Values may be sent and summed in bfloat16 or wider, within the bound.
A program may use at most 64 MiB of HBM per device.

```python
import math
import jax
import jax.numpy as jnp
from jax import lax

ORBITALS = 128
BLOCKS = 2
MODES = 4
REACH = 4
PASSES = 2
MOMENTA = 8
ENERGIES = 16


def draw_mode_shift(key, part):
    order = jax.random.permutation(jax.random.fold_in(key, 11), MODES)
    return (order % 3 - 1).astype(jnp.int32)


def draw_mode_offset(key, part):
    order = jax.random.permutation(jax.random.fold_in(key, 23), MODES)
    return (order % REACH + 1).astype(jnp.int32)


def plant(entries, own_key, least, high):
    dims = entries.shape
    place = [jax.random.randint(jax.random.fold_in(own_key, axis), (), 0, dims[axis]) for axis in range(len(dims))]
    entries = entries.at[tuple(place)].set(least)
    longest = dims.index(max(dims))
    place[longest] = (place[longest] + 1) % dims[longest]
    return entries.at[tuple(place)].set(high)


def block_scale(key, extent, split, low, largest):
    def one(position, shards_of):
        steps = jax.random.uniform(jax.random.fold_in(jax.random.fold_in(key, 6), position), (shards_of,), jnp.float32, low / len(split), largest / len(split))
        return jnp.repeat(jnp.exp(steps), extent[position] // shards_of).reshape((-1,) + (1,) * (len(extent) - position - 1))

    gain = one(*split[0])
    for cut in split[1:]:
        gain = gain * one(*cut)
    return gain


def noise(key, shape, width, limit, split=(), kind=jnp.bfloat16):
    array = width * jax.random.normal(key, shape, jnp.float32)
    if split:
        array = array * block_scale(key, shape, split, -0.22, 0.18)
    return jnp.clip(array, -limit, limit).astype(kind)


def setup_inputs(seed: int = 0) -> dict:
    streams_of = jax.random.split(jax.random.key(seed), 8)
    return {
        "green": noise(streams_of[0], (2, MOMENTA, ENERGIES, BLOCKS, ORBITALS, ORBITALS), ORBITALS ** -0.5, 0.5, ((1, 8), (2, 4))),
        "bare": noise(streams_of[1], (2, MOMENTA, ENERGIES, BLOCKS, ORBITALS, ORBITALS), ORBITALS ** -0.5, 0.5, ((1, 8), (2, 4))),
        "coupling": noise(streams_of[2], (MODES, ORBITALS, ORBITALS), (4 * ORBITALS) ** -0.5, 0.25),
        "occupation": jnp.clip(jnp.exp(jax.random.uniform(streams_of[3], (MODES,), jnp.float32, math.log(0.2), math.log(2.0))), 0.2, 2.0),
        "mode_shift": draw_mode_shift(jax.random.fold_in(streams_of[7], 71), 0),
        "mode_offset": draw_mode_offset(jax.random.fold_in(streams_of[7], 71), 0),
        "mode_block": plant(jax.random.randint(streams_of[6], (BLOCKS, MODES), 0, BLOCKS), jax.random.fold_in(streams_of[6], 1), 0, BLOCKS - 1).astype(jnp.int32),
    }


def complex_product(left_pair, right_pair):
    left_float = left_pair.astype(jnp.float32)
    right_float = right_pair.astype(jnp.float32)
    real_part = jnp.einsum("...ab,...bc->...ac", left_float[0], right_float[0]) - jnp.einsum("...ab,...bc->...ac", left_float[1], right_float[1])
    imag_part = jnp.einsum("...ab,...bc->...ac", left_float[0], right_float[1]) + jnp.einsum("...ab,...bc->...ac", left_float[1], right_float[0])
    return jnp.stack([real_part, imag_part])


def one_point(padded, bare, coupling, occupation, mode_shift, mode_offset, mode_block, kpoint):
    summed_terms = jnp.zeros((2, ENERGIES, BLOCKS, ORBITALS, ORBITALS), jnp.float32)

    def add_mode(mode_index, accum):
        source_index = ((kpoint - mode_shift[mode_index]) % MOMENTA).astype(jnp.int32)
        source = lax.dynamic_index_in_dim(padded, source_index, 1, keepdims=False)
        lower_side = lax.dynamic_slice_in_dim(source, (REACH - mode_offset[mode_index]).astype(jnp.int32), ENERGIES, 1)
        upper_side = lax.dynamic_slice_in_dim(source, (REACH + mode_offset[mode_index]).astype(jnp.int32), ENERGIES, 1)
        lower_side = jnp.take(lower_side, mode_block[:, mode_index], axis=2)
        upper_side = jnp.take(upper_side, mode_block[:, mode_index], axis=2)
        weight = occupation[mode_index]
        summed = (weight * lower_side.astype(jnp.float32) + (weight + 1.0) * upper_side.astype(jnp.float32)).astype(jnp.bfloat16)
        matrix = coupling[mode_index].astype(jnp.float32)
        coupled = jnp.einsum("ab,...bc->...ac", matrix, summed.astype(jnp.float32)).astype(jnp.bfloat16)
        contribution = jnp.einsum("...ab,cb->...ac", coupled.astype(jnp.float32), matrix)
        return accum + contribution

    sigma = lax.fori_loop(0, MODES, add_mode, summed_terms).astype(jnp.bfloat16)
    bare_point = lax.dynamic_index_in_dim(bare, kpoint, 1, keepdims=False)
    product = complex_product(bare_point, sigma).astype(jnp.bfloat16)
    correction = complex_product(product, bare_point)
    return (bare_point.astype(jnp.float32) + correction).astype(jnp.bfloat16)


def reference(green, bare, coupling, occupation, mode_shift, mode_offset, mode_block):
    current = green
    for pass_index in range(PASSES):
        padded = jnp.pad(current, ((0, 0), (0, 0), (REACH, REACH), (0, 0), (0, 0), (0, 0)))
        points = lax.map(lambda kpoint: one_point(padded, bare, coupling, occupation, mode_shift, mode_offset, mode_block, kpoint), jnp.arange(MOMENTA, dtype=jnp.int32))
        current = jnp.moveaxis(points, 0, 1)
    return current
```

```python
import functools

import jax
import jax.numpy as jnp
from jax import lax
from jax.experimental import pallas as pl
from jax.experimental.pallas import tpu as pltpu
from jax.sharding import PartitionSpec as P

MODES = 4
REACH = 4
PASSES = 2

FROM_NEXT, FROM_PREV, FROM_DOWN, FROM_UP = range(4)
OWN = 2

f32 = jnp.float32
bf16 = jnp.bfloat16

UPWARD = ((3, 2, 1, 0), (1, 3, 2, 0))
DOWNWARD = ((0, 1, 2, 3), (1, 0, 3, 2))
ACROSS = ((3, 0, 2, 1), (1, 0, 3, 2))

STEPS = (
    (
    (
        "Q10+Q20", "I3+U3", "Q11+Q00", "I0+D0", "Q21+Q30+Q12+Q01", "I2+U2", "Q22+Q31+Q13+S1", "Q02+Q03+S0",
        "I1+D1+U1", "Q23+Q32+U0+D3", "Q33+S3+D2", "S2", "O1+A1+O0+A0", "O3+A3+O2+A2", "C1", "C0", "C3", "C2",
    ),
    (
        "Q10+Q20", "Q02", "I1+Q13+Q31", "Q11+Q00+Q22", "I0+D0+D1", "Q21+Q30", "Q12+S1+Q01", "I3+U3", "Q33",
        "Q03+S0", "I2+U1+D3", "Q23+Q32+S3+U0", "S2+U2+D2", "O1+A1+O0+A0", "O3+A3+O2+A2", "C1", "C0", "C3",
        "C2",
    ),
    ),
    (
    (
        "Q10+Q20", "Q11+Q00", "Q21+Q30+Q12+Q01", "Q22+Q31", "I3+U3", "Q13+S1", "Q23+Q32", "I0+D0",
        "Q02+Q03+S0", "Q33+S3", "I2+U2+S2", "I1+D1+U1", "D3+U0", "D2", "O1+A1+O0+A0", "O3+A3+O2+A2", "C1",
        "C0", "C3", "C2",
    ),
    (
        "Q10+Q20", "Q02", "I1+Q13+Q31", "Q11+Q00+Q22", "I0+D0+D1", "Q21+Q30", "Q12+S1+Q01", "I3+U3", "Q33",
        "Q03+S0", "I2+U1+D3", "Q23+Q32+S3+U0", "S2+U2+D2", "O1+A1+O0+A0", "O3+A3+O2+A2", "C1", "C0", "C3",
        "C2",
    ),
    ),
)


def matmul(left, right):
    return jnp.dot(left, right, preferred_element_type=f32)


def side_by_side(*parts):
    return parts[0] if len(parts) == 1 else jnp.concatenate(parts, axis=1)


def on_top(*parts):
    return parts[0] if len(parts) == 1 else jnp.concatenate(parts, axis=0)


def kernel(
    mom_count, en_count, passes,
    occupation_hbm, mode_shift_hbm, mode_offset_hbm, mode_block_hbm, green, bare_hbm, coupling_hbm,
    out,
    occupation, mode_shift, mode_offset, mode_block, bare, coupling,
    matrices, matrices_t, share_t, own_t, wide_bare, real_coupled, below, above,
    share_own, part_own, real_current, low_rim, high_rim, imag_source,
    share_out, part_out, inbox,
    rim_sem, imag_sem, inbox_sem, send_sem, input_sem,
):
    energies = green.shape[2]
    blocks = green.shape[3]
    size = green.shape[4]
    k = lax.axis_index("mom")
    z = lax.axis_index("en")
    next_k = lax.rem(k + 1, mom_count)
    prev_k = lax.rem(k + mom_count - 1, mom_count)
    up_z = lax.rem(z + 1, en_count)
    down_z = lax.rem(z + en_count - 1, en_count)
    is_odd = lax.rem(k, 2) == 1
    is_even = lax.rem(k, 2) == 0
    has_up = z < en_count - 1
    has_down = z > 0

    barrier = pltpu.get_barrier_semaphore()
    for other in (next_k, prev_k):
        pl.semaphore_signal(
            barrier, inc=1, device_id={"mom": other}, device_id_type=pl.DeviceIdType.MESH
        )

    @pl.when(has_up)
    def _():
        pl.semaphore_signal(
            barrier, inc=1, device_id={"en": up_z}, device_id_type=pl.DeviceIdType.MESH
        )

    @pl.when(has_down)
    def _():
        pl.semaphore_signal(
            barrier, inc=1, device_id={"en": down_z}, device_id_type=pl.DeviceIdType.MESH
        )

    pairs = (
        (coupling_hbm, coupling),
        (bare_hbm, bare),
        (occupation_hbm, occupation),
        (mode_shift_hbm, mode_shift),
        (mode_offset_hbm, mode_offset),
        (mode_block_hbm, mode_block),
    )
    input_fetch = [
        pltpu.make_async_copy(there, here, input_sem.at[i]) for i, (there, here) in enumerate(pairs)
    ]
    green_fetch = [
        pltpu.make_async_copy(green.at[0, 0, e], real_current[0][e], input_sem.at[len(pairs)])
        for e in range(energies)
    ]
    green_fetch += [
        pltpu.make_async_copy(green.at[1, 0, e], imag_source[0][e].at[OWN], input_sem.at[len(pairs)])
        for e in range(energies)
    ]
    for fetch in green_fetch + input_fetch:
        fetch.start()

    pl.semaphore_wait(barrier, 2 + has_up.astype(jnp.int32) + has_down.astype(jnp.int32))

    pltpu.make_async_copy(bare, bare, input_sem.at[len(pairs)]).wait()

    def send(source, target, sent, landed, device):
        pltpu.make_async_remote_copy(
            src_ref=source,
            dst_ref=target,
            send_sem=sent,
            recv_sem=landed,
            device_id=device,
            device_id_type=pl.DeviceIdType.MESH,
        ).start()

    def across(source, targets, landed):
        return [
            lambda: send(source[0], targets[0], send_sem.at[0], landed, {"mom": next_k}),
            lambda: send(source[1], targets[1], send_sem.at[0], landed, {"mom": prev_k}),
        ]

    def imag_across(p, e):
        source = imag_source[p][e].at[OWN]
        slots = imag_source[p][e]
        return across((source, source), (slots.at[1], slots.at[0]), imag_sem.at[p, e])

    def start(actions):
        for action in actions:
            action()

    def send_up(source, target, landed):
        send(source, target, send_sem.at[1], landed, {"en": up_z})

    def send_down(source, target, landed):
        send(source, target, send_sem.at[2], landed, {"en": down_z})

    def send_real_up(p, e):
        send_up(real_current[p][e], low_rim[p][e], rim_sem.at[p, 0, e])

    def send_real_down(p, e):
        send_down(real_current[p][e], high_rim[p][e], rim_sem.at[p, 1, e])

    first = [imag_across(0, e) for e in ACROSS[0]]
    pl.when(is_odd)(lambda: start([ways[0] for ways in first]))
    pl.when(is_even)(lambda: start([ways[1] for ways in first]))
    pl.when(has_up)(lambda: [send_real_up(0, e) for e in UPWARD[0]] and None)
    pl.when(has_down)(lambda: [send_real_down(0, e) for e in DOWNWARD[0]] and None)
    pl.when(is_odd)(lambda: start([ways[1] for ways in first]))
    pl.when(is_even)(lambda: start([ways[0] for ways in first]))

    @pl.when(jnp.logical_not(has_down))
    def _():
        for p in range(passes):
            for j in range(energies):
                low_rim[p][j][...] = jnp.zeros_like(low_rim[p][j])
                inbox[p, j, FROM_DOWN] = jnp.zeros_like(inbox[p, j, FROM_DOWN])

    @pl.when(jnp.logical_not(has_up))
    def _():
        for p in range(passes):
            for j in range(energies):
                high_rim[p][j][...] = jnp.zeros_like(high_rim[p][j])
                inbox[p, j, FROM_UP] = jnp.zeros_like(inbox[p, j, FROM_UP])

    for fetch in input_fetch:
        fetch.wait()

    weight, shift, slot, picks = [], [], [], []
    for m in range(MODES):
        mode = jnp.int32(0)
        for j in range(1, MODES):
            mode = jnp.where(mode_offset[j] == m + 1, jnp.int32(j), mode)
        weight.append(occupation[mode])
        shift.append(mode_shift[mode])
        slot.append(jnp.where(shift[m] == 0, OWN, jnp.where(shift[m] > 0, 1, 0)))
        picks.append([mode_block[b, mode] for b in range(blocks)])
        matrix = coupling[mode]
        turned = matrix.astype(f32).T
        rows = pl.ds(m * size, size)
        matrices[m] = matrix
        matrices_t[rows, :] = turned.astype(bf16)
        for q, (kept_t, columns) in {
            1: (share_t, pl.ds(0, size)), -1: (share_t, pl.ds(size, size)), 0: (own_t, pl.ds(0, size)),
        }.items():
            kept = jnp.where(shift[m] == q, 1.0, 0.0).astype(f32)
            kept_t[rows, columns] = (turned * kept).astype(bf16)

    for e in range(energies):
        for b in range(blocks):
            real, imag = bare[0, 0, e, b], bare[1, 0, e, b]
            wide_bare[e, b, pl.ds(0, size), :] = side_by_side(real, imag)
            wide_bare[e, b, pl.ds(size, size), :] = side_by_side(-imag, real)

    waited, sends, closed = set(), [], []

    def in_turn(order, ready):
        return next((i for i, e in enumerate(order) if e not in ready), len(order))

    def later(condition, action):
        sends.append((condition, action))

    def later_across(ways):
        far, near = (0, 1) if parity else (1, 0)
        later("far", ways[far])
        later("near", ways[near])

    def send_all():
        for condition, guard in (("far", None), (has_up, has_up), (has_down, has_down), ("near", None)):
            actions = [action for wanted, action in sends if wanted is condition]
            if actions and guard is None:
                start(actions)
            elif actions:
                pl.when(guard)(functools.partial(start, actions))
        sends.clear()

    def landed_pair(sem, both, one):
        pl.when(jnp.logical_and(has_up, has_down))(lambda: pltpu.make_async_copy(both, both, sem).wait())
        pl.when(jnp.logical_xor(has_up, has_down))(lambda: pltpu.make_async_copy(one, one, sem).wait())

    def once(*key):
        fresh = key not in waited
        waited.add(key)
        return fresh

    def rim_landed(p, side, e):
        if once("rim", p, side, e):
            one = (low_rim, high_rim)[side][p][e]
            pl.when((has_down, has_up)[side])(lambda: pltpu.make_async_copy(one, one, rim_sem.at[p, side, e]).wait())

    def imag_landed(p, e):
        if once("imag", p, e):
            both = imag_source[p][e].at[pl.ds(0, 2)]
            pltpu.make_async_copy(both, both, imag_sem.at[p, e]).wait()

    def inbox_landed(p, e):
        if once("inbox", p, e):
            landed_pair(inbox_sem.at[p, e], inbox.at[p, e], inbox.at[p, e, pl.ds(0, 3)])

    def real_at(p, e, pick):
        if e < 0:
            return low_rim[p][e + energies][pick]
        if e >= energies:
            return high_rim[p][e - energies][pick]
        return real_current[p][e][pick]

    def rims_landed(p, e, m):
        if e - m - 1 < 0:
            rim_landed(p, 0, e - m - 1 + energies)
        if e + m + 1 >= energies:
            rim_landed(p, 1, e + m + 1 - energies)

    def mode_step(p, e, m):
        summed = []
        for b in range(blocks):
            low_side = real_at(p, e - m - 1, picks[m][b]).astype(f32)
            high_side = real_at(p, e + m + 1, picks[m][b]).astype(f32)
            mixed = weight[m] * low_side + (weight[m] + 1.0) * high_side
            summed.append(mixed.astype(bf16))
        coupled = matmul(matrices[m], side_by_side(*summed)).astype(bf16)
        for b in range(blocks):
            real_coupled[e, pl.ds(b * size, size), pl.ds(m * size, size)] = coupled[:, b * size:(b + 1) * size]

    def share_step(p, e):
        share = matmul(real_coupled[e], share_t[...]).astype(bf16)
        for way in range(2):
            for b in range(blocks):
                share_out[p][e, way, b] = share[b * size:(b + 1) * size, way * size:(way + 1) * size]
        later_across(across(
            (share_out[p].at[e, 0], share_out[p].at[e, 1]),
            (inbox.at[p, e, FROM_PREV], inbox.at[p, e, FROM_NEXT]), inbox_sem.at[p, e],
        ))

    def own_share_step(p, e):
        share_own[e] = matmul(real_coupled[e], own_t[...])

    def imag_step(p, e):
        for m in range(MODES):
            chosen = imag_source[p][e][slot[m]]
            coupled = matmul(matrices[m], side_by_side(*[chosen[c] for c in range(blocks)]))
            lower = (weight[m] * coupled).astype(bf16)
            upper = ((weight[m] + 1.0) * coupled).astype(bf16)
            for c in range(blocks):
                below[e, m, c] = lower[:, c * size:(c + 1) * size]
                above[e, m, c] = upper[:, c * size:(c + 1) * size]

    def part_of(target):
        lower = [m for m in range(MODES) if 0 <= target - m - 1 < energies]
        upper = [m for m in range(MODES) if 0 <= target + m + 1 < energies]
        rows = []
        for b in range(blocks):
            terms = [below[target - m - 1, m, picks[m][b]] for m in lower]
            terms += [above[target + m + 1, m, picks[m][b]] for m in upper]
            rows.append(side_by_side(*terms))
        spans = [
            matrices_t[pl.ds(ms[0] * size, len(ms) * size), :] for ms in (lower, upper) if ms
        ]
        return matmul(on_top(*rows), on_top(*spans))

    def part_step(p, e, up):
        part = part_of(e + energies if up else e - energies).astype(bf16)
        source = part_out[p].at[1 if up else 0, e]
        for b in range(blocks):
            part_out[p][1 if up else 0, e, b] = part[b * size:(b + 1) * size]
        if up:
            later(has_up, lambda: send_up(source, inbox.at[p, e, FROM_DOWN], inbox_sem.at[p, e]))
        else:
            later(has_down, lambda: send_down(source, inbox.at[p, e, FROM_UP], inbox_sem.at[p, e]))

    def own_part_step(p, e):
        part_own[e] = part_of(e)

    def close_step(p, e):
        for b in range(blocks):
            rows = slice(b * size, (b + 1) * size)
            real = share_own[e, rows] + inbox[p, e, FROM_NEXT, b].astype(f32)
            real = (real + inbox[p, e, FROM_PREV, b].astype(f32)).astype(bf16)
            imag = part_own[e, rows] + inbox[p, e, FROM_DOWN, b].astype(f32)
            imag = (imag + inbox[p, e, FROM_UP, b].astype(f32)).astype(bf16)
            sigma = on_top(side_by_side(real, imag), side_by_side(-imag, real))
            both = wide_bare[e, b, pl.ds(0, size), :]
            product = matmul(both, sigma).astype(bf16)
            new = (both.astype(f32) + matmul(product, wide_bare[e, b])).astype(bf16)
            if p == passes - 1:
                out[0, 0, e, b] = new[:, :size]
                out[1, 0, e, b] = new[:, size:]
            else:
                real_current[p + 1][e][b] = new[:, :size]
                imag_source[p + 1][e][OWN, b] = new[:, size:]
        if p < passes - 1:
            closed.append(e)
            for condition, order, action in ((None, ACROSS, imag_across), (has_up, UPWARD, send_real_up), (has_down, DOWNWARD, send_real_down)):
                begin, end = in_turn(order[p + 1], closed[:-1]), in_turn(order[p + 1], closed)
                for turn in order[p + 1][begin:end]:
                    if condition is None:
                        later_across(action(p + 1, turn))
                    else:
                        later(condition, functools.partial(action, p + 1, turn))

    steps = {
        "Q": mode_step, "S": share_step, "O": own_share_step, "I": imag_step,
        "U": functools.partial(part_step, up=True), "D": functools.partial(part_step, up=False),
        "A": own_part_step, "C": close_step,
    }
    waits = {"Q": rims_landed, "I": imag_landed, "C": inbox_landed}
    def run(odd):
        nonlocal parity
        parity = odd
        waited.clear()
        for p in range(passes):
            closed.clear()
            for group in STEPS[odd][p]:
                calls = [(name[0], [int(digit) for digit in name[1:]]) for name in group.split("+")]
                for kind, at in calls:
                    if kind in waits:
                        waits[kind](p, *at)
                for kind, at in calls:
                    steps[kind](p, *at)
                send_all()

    parity = 0
    pl.when(is_even)(lambda: run(0))
    pl.when(is_odd)(lambda: run(1))

    everything = inbox.at[0]
    pltpu.make_async_copy(inbox, inbox, send_sem.at[0]).wait()
    pl.when(has_up)(lambda: pltpu.make_async_copy(everything, everything, send_sem.at[1]).wait())
    pl.when(has_down)(lambda: pltpu.make_async_copy(everything, everything, send_sem.at[2]).wait())


def shards(mom_count, en_count, green, bare, coupling, occupation, mode_shift, mode_offset, mode_block):
    _, _, energies, blocks, size, _ = green.shape
    assert energies == REACH and coupling.shape[0] == MODES and MODES == REACH
    pair = (blocks, size, size)
    vmem = pltpu.VMEM
    smem = pltpu.SMEM
    dma = pltpu.SemaphoreType.DMA
    scratch = [
        smem(occupation.shape, occupation.dtype),
        smem(mode_shift.shape, mode_shift.dtype),
        smem(mode_offset.shape, mode_offset.dtype),
        smem(mode_block.shape, mode_block.dtype),
        vmem(bare.shape, bf16),
        vmem(coupling.shape, bf16),
        vmem((MODES, size, size), bf16),
        vmem((MODES * size, size), bf16),
        vmem((MODES * size, 2 * size), bf16),
        vmem((MODES * size, size), bf16),
        vmem((energies, blocks, 2 * size, 2 * size), bf16),
        vmem((energies, blocks * size, MODES * size), bf16),
        vmem((energies, MODES) + pair, bf16),
        vmem((energies, MODES) + pair, bf16),
        vmem((energies, blocks * size, size), f32),
        vmem((energies, blocks * size, size), f32),
        [[vmem(pair, bf16) for _ in range(energies)] for _ in range(PASSES)],
        [[vmem(pair, bf16) for _ in range(energies)] for _ in range(PASSES)],
        [[vmem(pair, bf16) for _ in range(energies)] for _ in range(PASSES)],
        [[vmem((3,) + pair, bf16) for _ in range(energies)] for _ in range(PASSES)],
        [vmem((energies, 2) + pair, bf16) for _ in range(PASSES)],
        [vmem((2, energies) + pair, bf16) for _ in range(PASSES)],
        vmem((PASSES, energies, 4) + pair, bf16),
        dma((PASSES, 2, energies)),
        dma((PASSES, energies)),
        dma((PASSES, energies)),
        dma((3,)),
        dma((7,)),
    ]
    whole = pl.BlockSpec(memory_space=pltpu.VMEM)
    anywhere = pl.BlockSpec(memory_space=pltpu.HBM)
    return pl.pallas_call(
        functools.partial(kernel, mom_count, en_count, PASSES),
        out_shape=jax.ShapeDtypeStruct(green.shape, green.dtype),
        in_specs=[anywhere] * 7,
        out_specs=whole,
        scratch_shapes=scratch,
        compiler_params=pltpu.CompilerParams(
            collective_id=0, has_side_effects=True, vmem_limit_bytes=40 * 1024 * 1024
        ),
        name="born_passes",
    )(*[pltpu.with_memory_space_constraint(a, pltpu.HBM) for a in (occupation, mode_shift, mode_offset, mode_block, green, bare, coupling)])


def solution(mesh):
    spread = P(None, "mom", "en", None, None, None)
    return jax.shard_map(
        functools.partial(shards, mesh.shape["mom"], mesh.shape["en"]),
        mesh=mesh,
        in_specs=(spread, spread, P(), P(), P(), P(), P()),
        out_specs=spread,
        check_vma=False,
    )
```

```python
import functools

import jax
import jax.numpy as jnp
from jax import lax
from jax.experimental import pallas as pl
from jax.experimental.pallas import tpu as pltpu
from jax.sharding import PartitionSpec as P

MODES = 4
REACH = 4
PASSES = 2

FROM_NEXT, FROM_PREV, FROM_DOWN, FROM_UP = range(4)
OWN = 2

f32 = jnp.float32
bf16 = jnp.bfloat16

UPWARD = ((3, 2, 1, 0), (1, 3, 2, 0))
DOWNWARD = ((0, 1, 2, 3), (1, 0, 3, 2))
ACROSS = ((3, 0, 2, 1), (1, 0, 3, 2))

STEPS = (
    (
    (
        "Q10+Q20", "J33+U3", "J30+J31+J32", "Q11+Q00", "J03+D0", "J00+J01+J02+Q21+Q30+Q12+Q01", "I2",
        "Q13+S1", "J13+D1+U1", "Q22+Q31+J10+J11+J12+Q02+Q03+S0+U0+D3", "Q32+Q33+S3", "Q23+S2+D2+U2",
        "O1+A1+O0+A0", "O3+A3+O2+A2", "C10", "C11", "C0", "C3", "C2",
    ),
    (
        "Q10+Q20", "Q02", "I1", "Q13+Q31", "J02+J03+D0+D1", "J00+J01+Q11+Q00+Q22", "Q12+S1", "J33+U3",
        "J30+J31+J32+Q21+Q30+Q01+Q33+Q03+S0", "J22+J23+U1+D3+D2", "J20+J21+Q23+Q32+S3+U0", "S2+U2",
        "O1+A1+O0+A0", "O3+A3+O2+A2", "C1", "C0", "C3", "C2",
    ),
    ),
    (
    (
        "Q10+Q20", "Q11+Q00", "Q21+Q30+Q12+Q01", "J33+U3", "J30+J31+J32+Q13+S1", "Q22+Q31", "J03+D0",
        "J00+J01+J02+Q02+Q03+S0", "Q23+Q32", "I2", "Q33+S3", "J13+D1+U1", "J10+J11+J12+S2+D3+U0", "D2+U2",
        "O1+A1+O0+A0", "O3+A3+O2+A2", "C10", "C11", "C0", "C3", "C2",
    ),
    (
        "Q10+Q20", "Q02", "I1", "Q13+Q31", "J02+J03+D0+D1", "J00+J01+Q11+Q00+Q22", "Q12+S1", "J33+U3",
        "J30+J31+J32+Q21+Q30+Q01+Q33+Q03+S0", "J22+J23+U1+D3+D2", "J20+J21+Q23+Q32+S3+U0", "S2+U2",
        "O1+A1+O0+A0", "O3+A3+O2+A2", "C1", "C0", "C3", "C2",
    ),
    ),
)


HALVED = ((1,), ())


def matmul(left, right):
    return jnp.dot(left, right, preferred_element_type=f32)


def side_by_side(*parts):
    return parts[0] if len(parts) == 1 else jnp.concatenate(parts, axis=1)


def on_top(*parts):
    return parts[0] if len(parts) == 1 else jnp.concatenate(parts, axis=0)


def kernel(
    mom_count, en_count, passes,
    occupation_hbm, mode_shift_hbm, mode_offset_hbm, mode_block_hbm, green, bare_hbm, coupling_hbm,
    out,
    occupation, mode_shift, mode_offset, mode_block, bare, coupling,
    matrices, matrices_t, share_t, own_t, wide_bare, real_coupled, below, above,
    share_own, part_own, real_current, low_rim, high_rim, imag_source,
    share_out, part_out, inbox,
    rim_sem, imag_sem, inbox_sem, send_sem, input_sem,
):
    energies = green.shape[2]
    blocks = green.shape[3]
    size = green.shape[4]
    k = lax.axis_index("mom")
    z = lax.axis_index("en")
    next_k = lax.rem(k + 1, mom_count)
    prev_k = lax.rem(k + mom_count - 1, mom_count)
    up_z = lax.rem(z + 1, en_count)
    down_z = lax.rem(z + en_count - 1, en_count)
    is_odd = lax.rem(k, 2) == 1
    is_even = lax.rem(k, 2) == 0
    has_up = z < en_count - 1
    has_down = z > 0

    barrier = pltpu.get_barrier_semaphore()
    for other in (next_k, prev_k):
        pl.semaphore_signal(
            barrier, inc=1, device_id={"mom": other}, device_id_type=pl.DeviceIdType.MESH
        )

    @pl.when(has_up)
    def _():
        pl.semaphore_signal(
            barrier, inc=1, device_id={"en": up_z}, device_id_type=pl.DeviceIdType.MESH
        )

    @pl.when(has_down)
    def _():
        pl.semaphore_signal(
            barrier, inc=1, device_id={"en": down_z}, device_id_type=pl.DeviceIdType.MESH
        )

    pairs = (
        (coupling_hbm, coupling),
        (bare_hbm, bare),
        (occupation_hbm, occupation),
        (mode_shift_hbm, mode_shift),
        (mode_offset_hbm, mode_offset),
        (mode_block_hbm, mode_block),
    )
    input_fetch = [
        pltpu.make_async_copy(there, here, input_sem.at[i]) for i, (there, here) in enumerate(pairs)
    ]
    green_fetch = [
        pltpu.make_async_copy(green.at[0, 0, e], real_current[0][e], input_sem.at[len(pairs)])
        for e in range(energies)
    ]
    green_fetch += [
        pltpu.make_async_copy(green.at[1, 0, e], imag_source[0][e].at[OWN], input_sem.at[len(pairs)])
        for e in range(energies)
    ]
    for fetch in green_fetch + input_fetch:
        fetch.start()

    pl.semaphore_wait(barrier, 2 + has_up.astype(jnp.int32) + has_down.astype(jnp.int32))

    pltpu.make_async_copy(bare, bare, input_sem.at[len(pairs)]).wait()

    def send(source, target, sent, landed, device):
        pltpu.make_async_remote_copy(
            src_ref=source,
            dst_ref=target,
            send_sem=sent,
            recv_sem=landed,
            device_id=device,
            device_id_type=pl.DeviceIdType.MESH,
        ).start()

    def across(source, targets, landed):
        return [
            lambda: send(source[0], targets[0], send_sem.at[0], landed, {"mom": next_k}),
            lambda: send(source[1], targets[1], send_sem.at[0], landed, {"mom": prev_k}),
        ]

    def imag_across(p, e, rows=slice(None)):
        source = part_ref(imag_source[p][e].at[OWN], rows)
        targets = part_ref(imag_source[p][e].at[1], rows), part_ref(imag_source[p][e].at[0], rows)
        return across((source, source), targets, imag_sem.at[p, e])

    def part_ref(ref, rows):
        return ref if rows == slice(None) else ref.at[rows]

    def pieces(p, e):
        return [slice(b, b + 1) for b in range(blocks)] if e in HALVED[p] else [slice(None)]

    def inbox_landing(p, e, piece):
        extra = [(q, x) for q in range(passes) for x in HALVED[q]]
        return inbox_sem.at[passes * energies + extra.index((p, e)) if piece else p * energies + e]

    def start(actions):
        for action in actions:
            action()

    def send_up(source, target, landed):
        send(source, target, send_sem.at[1], landed, {"en": up_z})

    def send_down(source, target, landed):
        send(source, target, send_sem.at[2], landed, {"en": down_z})

    def send_real_up(p, e, rows=slice(None)):
        send_up(part_ref(real_current[p][e], rows), part_ref(low_rim[p][e], rows), rim_sem.at[p, 0, e])

    def send_real_down(p, e, rows=slice(None)):
        send_down(part_ref(real_current[p][e], rows), part_ref(high_rim[p][e], rows), rim_sem.at[p, 1, e])

    first = [imag_across(0, e) for e in ACROSS[0]]
    pl.when(is_odd)(lambda: start([ways[0] for ways in first]))
    pl.when(is_even)(lambda: start([ways[1] for ways in first]))
    pl.when(has_up)(lambda: [send_real_up(0, e) for e in UPWARD[0]] and None)
    pl.when(has_down)(lambda: [send_real_down(0, e) for e in DOWNWARD[0]] and None)
    pl.when(is_odd)(lambda: start([ways[1] for ways in first]))
    pl.when(is_even)(lambda: start([ways[0] for ways in first]))

    @pl.when(jnp.logical_not(has_down))
    def _():
        for p in range(passes):
            for j in range(energies):
                low_rim[p][j][...] = jnp.zeros_like(low_rim[p][j])
                inbox[p, j, FROM_DOWN] = jnp.zeros_like(inbox[p, j, FROM_DOWN])

    @pl.when(jnp.logical_not(has_up))
    def _():
        for p in range(passes):
            for j in range(energies):
                high_rim[p][j][...] = jnp.zeros_like(high_rim[p][j])
                inbox[p, j, FROM_UP] = jnp.zeros_like(inbox[p, j, FROM_UP])

    for fetch in input_fetch:
        fetch.wait()

    weight, shift, slot, picks = [], [], [], []
    for m in range(MODES):
        mode = jnp.int32(0)
        for j in range(1, MODES):
            mode = jnp.where(mode_offset[j] == m + 1, jnp.int32(j), mode)
        weight.append(occupation[mode])
        shift.append(mode_shift[mode])
        slot.append(jnp.where(shift[m] == 0, OWN, jnp.where(shift[m] > 0, 1, 0)))
        picks.append([mode_block[b, mode] for b in range(blocks)])
        matrix = coupling[mode]
        turned = matrix.astype(f32).T
        rows = pl.ds(m * size, size)
        matrices[m] = matrix
        matrices_t[rows, :] = turned.astype(bf16)
        for q, (kept_t, columns) in {
            1: (share_t, pl.ds(0, size)), -1: (share_t, pl.ds(size, size)), 0: (own_t, pl.ds(0, size)),
        }.items():
            kept = jnp.where(shift[m] == q, 1.0, 0.0).astype(f32)
            kept_t[rows, columns] = (turned * kept).astype(bf16)

    for e in range(energies):
        for b in range(blocks):
            real, imag = bare[0, 0, e, b], bare[1, 0, e, b]
            wide_bare[e, b, pl.ds(0, size), :] = side_by_side(real, imag)
            wide_bare[e, b, pl.ds(size, size), :] = side_by_side(-imag, real)

    waited, sends, closed = set(), [], []

    def in_turn(order, ready):
        return next((i for i, e in enumerate(order) if e not in ready), len(order))

    def later(condition, action):
        sends.append((condition, action))

    def later_across(ways):
        far, near = (0, 1) if parity else (1, 0)
        later("far", ways[far])
        later("near", ways[near])

    def send_all():
        for condition, guard in (("far", None), (has_up, has_up), (has_down, has_down), ("near", None)):
            actions = [action for wanted, action in sends if wanted is condition]
            if actions and guard is None:
                start(actions)
            elif actions:
                pl.when(guard)(functools.partial(start, actions))
        sends.clear()

    def landed_pair(sem, both, one):
        pl.when(jnp.logical_and(has_up, has_down))(lambda: pltpu.make_async_copy(both, both, sem).wait())
        pl.when(jnp.logical_xor(has_up, has_down))(lambda: pltpu.make_async_copy(one, one, sem).wait())

    def once(*key):
        fresh = key not in waited
        waited.add(key)
        return fresh

    def rim_landed(p, side, e):
        if once("rim", p, side, e):
            one = (low_rim, high_rim)[side][p][e]
            pl.when((has_down, has_up)[side])(lambda: pltpu.make_async_copy(one, one, rim_sem.at[p, side, e]).wait())

    def imag_landed(p, e, m=None):
        if once("imag", p, e):
            both = imag_source[p][e].at[pl.ds(0, 2)]
            pltpu.make_async_copy(both, both, imag_sem.at[p, e]).wait()

    def inbox_landed(p, e, piece=0):
        rows = pieces(p, e)[piece]
        landed_pair(
            inbox_landing(p, e, piece),
            inbox.at[p, e, :, rows] if rows != slice(None) else inbox.at[p, e],
            inbox.at[p, e, pl.ds(0, 3), rows] if rows != slice(None) else inbox.at[p, e, pl.ds(0, 3)],
        )

    def real_at(p, e, pick):
        if e < 0:
            return low_rim[p][e + energies][pick]
        if e >= energies:
            return high_rim[p][e - energies][pick]
        return real_current[p][e][pick]

    def rims_landed(p, e, m):
        if e - m - 1 < 0:
            rim_landed(p, 0, e - m - 1 + energies)
        if e + m + 1 >= energies:
            rim_landed(p, 1, e + m + 1 - energies)

    def mode_step(p, e, m):
        summed = []
        for b in range(blocks):
            low_side = real_at(p, e - m - 1, picks[m][b]).astype(f32)
            high_side = real_at(p, e + m + 1, picks[m][b]).astype(f32)
            mixed = weight[m] * low_side + (weight[m] + 1.0) * high_side
            summed.append(mixed.astype(bf16))
        coupled = matmul(matrices[m], side_by_side(*summed)).astype(bf16)
        for b in range(blocks):
            real_coupled[e, pl.ds(b * size, size), pl.ds(m * size, size)] = coupled[:, b * size:(b + 1) * size]

    def share_step(p, e):
        share = matmul(real_coupled[e], share_t[...]).astype(bf16)
        for way in range(2):
            for b in range(blocks):
                share_out[p][e, way, b] = share[b * size:(b + 1) * size, way * size:(way + 1) * size]
        for piece, rows in enumerate(pieces(p, e)):
            later_across(across(
                (part_ref(share_out[p].at[e, 0], rows), part_ref(share_out[p].at[e, 1], rows)),
                (part_ref(inbox.at[p, e, FROM_PREV], rows), part_ref(inbox.at[p, e, FROM_NEXT], rows)),
                inbox_landing(p, e, piece),
            ))

    def own_share_step(p, e):
        share_own[e] = matmul(real_coupled[e], own_t[...])

    def imag_mode_step(p, e, m):
        chosen = imag_source[p][e][slot[m]]
        coupled = matmul(matrices[m], side_by_side(*[chosen[c] for c in range(blocks)]))
        lower = (weight[m] * coupled).astype(bf16)
        upper = ((weight[m] + 1.0) * coupled).astype(bf16)
        for c in range(blocks):
            below[e, m, c] = lower[:, c * size:(c + 1) * size]
            above[e, m, c] = upper[:, c * size:(c + 1) * size]

    def imag_step(p, e):
        for m in range(MODES):
            imag_mode_step(p, e, m)

    def part_of(target):
        lower = [m for m in range(MODES) if 0 <= target - m - 1 < energies]
        upper = [m for m in range(MODES) if 0 <= target + m + 1 < energies]
        rows = []
        for b in range(blocks):
            terms = [below[target - m - 1, m, picks[m][b]] for m in lower]
            terms += [above[target + m + 1, m, picks[m][b]] for m in upper]
            rows.append(side_by_side(*terms))
        spans = [
            matrices_t[pl.ds(ms[0] * size, len(ms) * size), :] for ms in (lower, upper) if ms
        ]
        return matmul(on_top(*rows), on_top(*spans))

    def part_step(p, e, up):
        part = part_of(e + energies if up else e - energies).astype(bf16)
        source = part_out[p].at[1 if up else 0, e]
        for b in range(blocks):
            part_out[p][1 if up else 0, e, b] = part[b * size:(b + 1) * size]
        condition, send_part, place = (has_up, send_up, FROM_DOWN) if up else (has_down, send_down, FROM_UP)
        for piece, rows in enumerate(pieces(p, e)):
            later(condition, functools.partial(
                send_part, part_ref(source, rows), part_ref(inbox.at[p, e, place], rows), inbox_landing(p, e, piece)
            ))

    def own_part_step(p, e):
        part_own[e] = part_of(e)

    def close_step(p, e, piece=0):
        halved = e in HALVED[p]
        for b in [piece] if halved else range(blocks):
            rows = slice(b * size, (b + 1) * size)
            real = share_own[e, rows] + inbox[p, e, FROM_NEXT, b].astype(f32)
            real = (real + inbox[p, e, FROM_PREV, b].astype(f32)).astype(bf16)
            imag = part_own[e, rows] + inbox[p, e, FROM_DOWN, b].astype(f32)
            imag = (imag + inbox[p, e, FROM_UP, b].astype(f32)).astype(bf16)
            sigma = on_top(side_by_side(real, imag), side_by_side(-imag, real))
            both = wide_bare[e, b, pl.ds(0, size), :]
            product = matmul(both, sigma).astype(bf16)
            new = (both.astype(f32) + matmul(product, wide_bare[e, b])).astype(bf16)
            if p == passes - 1:
                out[0, 0, e, b] = new[:, :size]
                out[1, 0, e, b] = new[:, size:]
            else:
                real_current[p + 1][e][b] = new[:, :size]
                imag_source[p + 1][e][OWN, b] = new[:, size:]
        if p == passes - 1:
            return
        if halved:
            rows = pieces(p, e)[piece]
            later_across(imag_across(p + 1, e, rows))
            later(has_up, functools.partial(send_real_up, p + 1, e, rows))
            later(has_down, functools.partial(send_real_down, p + 1, e, rows))
            if piece == 0:
                closed.append(e)
            return
        closed.append(e)
        for condition, order, action in ((None, ACROSS, imag_across), (has_up, UPWARD, send_real_up), (has_down, DOWNWARD, send_real_down)):
            begin, end = in_turn(order[p + 1], closed[:-1]), in_turn(order[p + 1], closed)
            for turn in order[p + 1][begin:end]:
                if condition is None:
                    later_across(action(p + 1, turn))
                else:
                    later(condition, functools.partial(action, p + 1, turn))

    steps = {
        "Q": mode_step, "S": share_step, "O": own_share_step, "I": imag_step, "J": imag_mode_step,
        "U": functools.partial(part_step, up=True), "D": functools.partial(part_step, up=False),
        "A": own_part_step, "C": close_step,
    }
    waits = {"Q": rims_landed, "I": imag_landed, "J": imag_landed, "C": inbox_landed}
    def run(odd):
        nonlocal parity
        parity = odd
        waited.clear()
        for p in range(passes):
            closed.clear()
            for group in STEPS[odd][p]:
                calls = [(name[0], [int(digit) for digit in name[1:]]) for name in group.split("+")]
                for kind, at in calls:
                    if kind in waits:
                        waits[kind](p, *at)
                for kind, at in calls:
                    steps[kind](p, *at)
                send_all()

    parity = 0
    pl.when(is_even)(lambda: run(0))
    pl.when(is_odd)(lambda: run(1))

    everything = inbox.at[0]
    pltpu.make_async_copy(inbox, inbox, send_sem.at[0]).wait()
    pl.when(has_up)(lambda: pltpu.make_async_copy(everything, everything, send_sem.at[1]).wait())
    pl.when(has_down)(lambda: pltpu.make_async_copy(everything, everything, send_sem.at[2]).wait())


def shards(mom_count, en_count, green, bare, coupling, occupation, mode_shift, mode_offset, mode_block):
    _, _, energies, blocks, size, _ = green.shape
    assert energies == REACH and coupling.shape[0] == MODES and MODES == REACH
    pair = (blocks, size, size)
    vmem = pltpu.VMEM
    smem = pltpu.SMEM
    dma = pltpu.SemaphoreType.DMA
    scratch = [
        smem(occupation.shape, occupation.dtype),
        smem(mode_shift.shape, mode_shift.dtype),
        smem(mode_offset.shape, mode_offset.dtype),
        smem(mode_block.shape, mode_block.dtype),
        vmem(bare.shape, bf16),
        vmem(coupling.shape, bf16),
        vmem((MODES, size, size), bf16),
        vmem((MODES * size, size), bf16),
        vmem((MODES * size, 2 * size), bf16),
        vmem((MODES * size, size), bf16),
        vmem((energies, blocks, 2 * size, 2 * size), bf16),
        vmem((energies, blocks * size, MODES * size), bf16),
        vmem((energies, MODES) + pair, bf16),
        vmem((energies, MODES) + pair, bf16),
        vmem((energies, blocks * size, size), f32),
        vmem((energies, blocks * size, size), f32),
        [[vmem(pair, bf16) for _ in range(energies)] for _ in range(PASSES)],
        [[vmem(pair, bf16) for _ in range(energies)] for _ in range(PASSES)],
        [[vmem(pair, bf16) for _ in range(energies)] for _ in range(PASSES)],
        [[vmem((3,) + pair, bf16) for _ in range(energies)] for _ in range(PASSES)],
        [vmem((energies, 2) + pair, bf16) for _ in range(PASSES)],
        [vmem((2, energies) + pair, bf16) for _ in range(PASSES)],
        vmem((PASSES, energies, 4) + pair, bf16),
        dma((PASSES, 2, energies)),
        dma((PASSES, energies)),
        dma((PASSES * energies + sum(map(len, HALVED)),)),
        dma((3,)),
        dma((7,)),
    ]
    whole = pl.BlockSpec(memory_space=pltpu.VMEM)
    anywhere = pl.BlockSpec(memory_space=pltpu.HBM)
    return pl.pallas_call(
        functools.partial(kernel, mom_count, en_count, PASSES),
        out_shape=jax.ShapeDtypeStruct(green.shape, green.dtype),
        in_specs=[anywhere] * 7,
        out_specs=whole,
        scratch_shapes=scratch,
        compiler_params=pltpu.CompilerParams(
            collective_id=0, has_side_effects=True, vmem_limit_bytes=40 * 1024 * 1024
        ),
        name="born_passes",
    )(*[pltpu.with_memory_space_constraint(a, pltpu.HBM) for a in (occupation, mode_shift, mode_offset, mode_block, green, bare, coupling)])


def solution(mesh):
    spread = P(None, "mom", "en", None, None, None)
    return jax.shard_map(
        functools.partial(shards, mesh.shape["mom"], mesh.shape["en"]),
        mesh=mesh,
        in_specs=(spread, spread, P(), P(), P(), P(), P()),
        out_specs=spread,
        check_vma=False,
    )
```

```python
import functools

import jax
import jax.numpy as jnp
from jax import lax
from jax.experimental import pallas as pl
from jax.experimental.pallas import tpu as pltpu
from jax.sharding import PartitionSpec as P

MODES = 4
REACH = 4
PASSES = 2

FROM_NEXT, FROM_PREV, FROM_DOWN, FROM_UP = range(4)
OWN = 2

f32 = jnp.float32
bf16 = jnp.bfloat16

UPWARD = ((3, 2, 1, 0), (1, 3, 2, 0))
DOWNWARD = ((0, 1, 2, 3), (1, 0, 3, 2))
ACROSS = ((3, 0, 2, 1), (1, 0, 3, 2))

STEPS = (
    (
    (
        "Q10+Q20", "J33+U3", "J30+J31+J32", "Q11+Q00", "J03+D0", "J00+J01+J02+Q21+Q30+Q12+Q01", "I2",
        "Q13+S1", "J13+D1+U1", "Q22+Q31+J10+J11+J12+Q02+Q03+S0+U0+D3", "Q32+Q33+S3", "Q23+S2+D2+U2",
        "O1+A1+O0+A0", "O3+A3+O2+A2", "C10", "C11", "C0", "C3", "C2",
    ),
    (
        "Q10+Q20", "Q02", "I1", "Q13+Q31", "J02+J03+D0+D1", "J00+J01+Q11+Q00+Q22", "Q12+S1", "Q01", "J33+U3",
        "J30+J31+J32+Q03+S0", "Q21+Q30+Q33", "J22+J23+U1+D3+D2", "J20+J21+Q23+Q32+S3+U0", "S2+U2",
        "O1+A1+O0+A0", "O3+A3+O2+A2", "C1", "C0", "C3", "C2",
    ),
    ),
    (
    (
        "Q10+Q20", "Q11+Q00", "Q21+Q30+Q12+Q01", "J33+U3", "J30+J31+J32+Q13+S1", "Q22+Q31", "J03+D0",
        "J00+J01+J02+Q02+Q03+S0", "Q23+Q32", "I2", "Q33+S3", "J13+D1+U1", "J10+J11+J12+S2+D3+U0", "D2+U2",
        "O1+A1+O0+A0", "O3+A3+O2+A2", "C10", "C11", "C0", "C3", "C2",
    ),
    (
        "Q10+Q20", "Q02", "I1", "Q13+Q31", "J02+J03+D0+D1", "J00+J01+Q11+Q00+Q22", "Q12+S1", "Q01", "J33+U3",
        "J30+J31+J32+Q03+S0", "Q21+Q30+Q33", "J22+J23+U1+D3+D2", "J20+J21+Q23+Q32+S3+U0", "S2+U2",
        "O1+A1+O0+A0", "O3+A3+O2+A2", "C1", "C0", "C3", "C2",
    ),
    ),
)


HALVED = ((1,), ())

IMAG_SLOT = ((0, 1, 2, 3), (0, 3, 1, 2))
LOW_SLOT = ((0, 1, 2, 3), (0, 3, 1, 2))
HIGH_SLOT = ((0, 1, 2, 3), (1, 0, 2, 4))


def matmul(left, right):
    return jnp.dot(left, right, preferred_element_type=f32)


def side_by_side(*parts):
    return parts[0] if len(parts) == 1 else jnp.concatenate(parts, axis=1)


def on_top(*parts):
    return parts[0] if len(parts) == 1 else jnp.concatenate(parts, axis=0)


def kernel(
    mom_count, en_count, passes,
    occupation_hbm, mode_shift_hbm, mode_offset_hbm, mode_block_hbm, green, bare_hbm, coupling_hbm,
    out,
    occupation, mode_shift, mode_offset, mode_block, bare, coupling,
    matrices, matrices_t, share_t, own_t, wide_bare, real_coupled, below, above,
    share_own, part_own, real_current, low_rim, high_rim, imag_source,
    share_out, part_out, inbox,
    rim_sem, imag_sem, inbox_sem, send_sem, input_sem,
):
    energies = green.shape[2]
    blocks = green.shape[3]
    size = green.shape[4]
    k = lax.axis_index("mom")
    z = lax.axis_index("en")
    next_k = lax.rem(k + 1, mom_count)
    prev_k = lax.rem(k + mom_count - 1, mom_count)
    up_z = lax.rem(z + 1, en_count)
    down_z = lax.rem(z + en_count - 1, en_count)
    is_odd = lax.rem(k, 2) == 1
    is_even = lax.rem(k, 2) == 0
    has_up = z < en_count - 1
    has_down = z > 0

    barrier = pltpu.get_barrier_semaphore()
    for other in (next_k, prev_k):
        pl.semaphore_signal(
            barrier, inc=1, device_id={"mom": other}, device_id_type=pl.DeviceIdType.MESH
        )

    @pl.when(has_up)
    def _():
        pl.semaphore_signal(
            barrier, inc=1, device_id={"en": up_z}, device_id_type=pl.DeviceIdType.MESH
        )

    @pl.when(has_down)
    def _():
        pl.semaphore_signal(
            barrier, inc=1, device_id={"en": down_z}, device_id_type=pl.DeviceIdType.MESH
        )

    pairs = (
        (coupling_hbm, coupling),
        (occupation_hbm, occupation),
        (mode_shift_hbm, mode_shift),
        (mode_offset_hbm, mode_offset),
        (mode_block_hbm, mode_block),
    )
    input_fetch = [
        pltpu.make_async_copy(there, here, input_sem.at[i]) for i, (there, here) in enumerate(pairs)
    ]
    green_fetch = [
        pltpu.make_async_copy(green.at[0, 0, e], real_current[0][e], input_sem.at[len(pairs)])
        for e in range(energies)
    ]
    green_fetch += [
        pltpu.make_async_copy(green.at[1, 0, e], imag_source[0][e].at[OWN], input_sem.at[len(pairs)])
        for e in range(energies)
    ]
    green_fetch += [pltpu.make_async_copy(bare_hbm, bare, input_sem.at[len(pairs)])]
    for fetch in green_fetch + input_fetch:
        fetch.start()

    pl.semaphore_wait(barrier, 2 + has_up.astype(jnp.int32) + has_down.astype(jnp.int32))

    pltpu.make_async_copy(inbox.at[0], inbox.at[0], input_sem.at[len(pairs)]).wait()

    def send(source, target, sent, landed, device):
        pltpu.make_async_remote_copy(
            src_ref=source,
            dst_ref=target,
            send_sem=sent,
            recv_sem=landed,
            device_id=device,
            device_id_type=pl.DeviceIdType.MESH,
        ).start()

    def across(source, targets, landed):
        return [
            lambda: send(source[0], targets[0], send_sem.at[0], landed, {"mom": next_k}),
            lambda: send(source[1], targets[1], send_sem.at[0], landed, {"mom": prev_k}),
        ]

    def imag_across(p, e, rows=slice(None)):
        source = part_ref(imag_source[p][e].at[OWN], rows)
        targets = part_ref(imag_source[p][e].at[1], rows), part_ref(imag_source[p][e].at[0], rows)
        return across((source, source), targets, imag_sem.at[IMAG_SLOT[p][e]])

    def part_ref(ref, rows):
        return ref if rows == slice(None) else ref.at[rows]

    def pieces(p, e):
        return [slice(b, b + 1) for b in range(blocks)] if e in HALVED[p] else [slice(None)]

    def inbox_landing(p, e, piece):
        extra = [(q, x) for q in range(passes) for x in HALVED[q]]
        return inbox_sem.at[passes * energies + extra.index((p, e)) if piece else p * energies + e]

    def start(actions):
        for action in actions:
            action()

    def send_up(source, target, landed):
        send(source, target, send_sem.at[1], landed, {"en": up_z})

    def send_down(source, target, landed):
        send(source, target, send_sem.at[2], landed, {"en": down_z})

    def send_real_up(p, e, rows=slice(None)):
        send_up(part_ref(real_current[p][e], rows), part_ref(low_rim[p][e], rows), rim_sem.at[0, LOW_SLOT[p][e]])

    def send_real_down(p, e, rows=slice(None)):
        send_down(part_ref(real_current[p][e], rows), part_ref(high_rim[p][e], rows), rim_sem.at[1, HIGH_SLOT[p][e]])

    first = [imag_across(0, e) for e in ACROSS[0]]
    pl.when(is_odd)(lambda: start([ways[0] for ways in first]))
    pl.when(is_even)(lambda: start([ways[1] for ways in first]))
    pl.when(has_up)(lambda: [send_real_up(0, e) for e in UPWARD[0]] and None)
    pl.when(has_down)(lambda: [send_real_down(0, e) for e in DOWNWARD[0]] and None)
    pl.when(is_odd)(lambda: start([ways[1] for ways in first]))
    pl.when(is_even)(lambda: start([ways[0] for ways in first]))

    @pl.when(jnp.logical_not(has_down))
    def _():
        for p in range(passes):
            for j in range(energies):
                low_rim[p][j][...] = jnp.zeros_like(low_rim[p][j])
                inbox[p, j, FROM_DOWN] = jnp.zeros_like(inbox[p, j, FROM_DOWN])

    @pl.when(jnp.logical_not(has_up))
    def _():
        for p in range(passes):
            for j in range(energies):
                high_rim[p][j][...] = jnp.zeros_like(high_rim[p][j])
                inbox[p, j, FROM_UP] = jnp.zeros_like(inbox[p, j, FROM_UP])

    for fetch in input_fetch:
        fetch.wait()

    weight, shift, slot, picks = [], [], [], []
    for m in range(MODES):
        mode = jnp.int32(0)
        for j in range(1, MODES):
            mode = jnp.where(mode_offset[j] == m + 1, jnp.int32(j), mode)
        weight.append(occupation[mode])
        shift.append(mode_shift[mode])
        slot.append(jnp.where(shift[m] == 0, OWN, jnp.where(shift[m] > 0, 1, 0)))
        picks.append([mode_block[b, mode] for b in range(blocks)])
        matrix = coupling[mode]
        turned = matrix.astype(f32).T
        rows = pl.ds(m * size, size)
        matrices[m] = matrix
        matrices_t[rows, :] = turned.astype(bf16)
        for q, (kept_t, columns) in {
            1: (share_t, pl.ds(0, size)), -1: (share_t, pl.ds(size, size)), 0: (own_t, pl.ds(0, size)),
        }.items():
            kept = jnp.where(shift[m] == q, 1.0, 0.0).astype(f32)
            kept_t[rows, columns] = (turned * kept).astype(bf16)

    for e in range(energies):
        for b in range(blocks):
            real, imag = bare[0, 0, e, b], bare[1, 0, e, b]
            wide_bare[e, b, pl.ds(0, size), :] = side_by_side(real, imag)
            wide_bare[e, b, pl.ds(size, size), :] = side_by_side(-imag, real)

    waited, sends, closed = set(), [], []

    def in_turn(order, ready):
        return next((i for i, e in enumerate(order) if e not in ready), len(order))

    def later(condition, action):
        sends.append((condition, action))

    def later_across(ways):
        far, near = (0, 1) if parity else (1, 0)
        later("far", ways[far])
        later("near", ways[near])

    def send_all():
        for condition, guard in (("far", None), (has_up, has_up), (has_down, has_down), ("near", None)):
            actions = [action for wanted, action in sends if wanted is condition]
            if actions and guard is None:
                start(actions)
            elif actions:
                pl.when(guard)(functools.partial(start, actions))
        sends.clear()

    def landed_pair(sem, both, one):
        pl.when(jnp.logical_and(has_up, has_down))(lambda: pltpu.make_async_copy(both, both, sem).wait())
        pl.when(jnp.logical_xor(has_up, has_down))(lambda: pltpu.make_async_copy(one, one, sem).wait())

    def once(*key):
        fresh = key not in waited
        waited.add(key)
        return fresh

    def rim_landed(p, side, e):
        if once("rim", p, side, e):
            one = (low_rim, high_rim)[side][p][e]
            pl.when((has_down, has_up)[side])(lambda: pltpu.make_async_copy(one, one, rim_sem.at[side, (LOW_SLOT, HIGH_SLOT)[side][p][e]]).wait())

    def imag_landed(p, e, m=None):
        if once("imag", p, e):
            both = imag_source[p][e].at[pl.ds(0, 2)]
            pltpu.make_async_copy(both, both, imag_sem.at[IMAG_SLOT[p][e]]).wait()

    def inbox_landed(p, e, piece=0):
        rows = pieces(p, e)[piece]
        landed_pair(
            inbox_landing(p, e, piece),
            inbox.at[p, e, :, rows] if rows != slice(None) else inbox.at[p, e],
            inbox.at[p, e, pl.ds(0, 3), rows] if rows != slice(None) else inbox.at[p, e, pl.ds(0, 3)],
        )

    def real_at(p, e, pick):
        if e < 0:
            return low_rim[p][e + energies][pick]
        if e >= energies:
            return high_rim[p][e - energies][pick]
        return real_current[p][e][pick]

    def rims_landed(p, e, m):
        if e - m - 1 < 0:
            rim_landed(p, 0, e - m - 1 + energies)
        if e + m + 1 >= energies:
            rim_landed(p, 1, e + m + 1 - energies)

    def mode_step(p, e, m):
        summed = []
        for b in range(blocks):
            low_side = real_at(p, e - m - 1, picks[m][b]).astype(f32)
            high_side = real_at(p, e + m + 1, picks[m][b]).astype(f32)
            mixed = weight[m] * low_side + (weight[m] + 1.0) * high_side
            summed.append(mixed.astype(bf16))
        coupled = matmul(matrices[m], side_by_side(*summed)).astype(bf16)
        for b in range(blocks):
            real_coupled[e, pl.ds(b * size, size), pl.ds(m * size, size)] = coupled[:, b * size:(b + 1) * size]

    def share_step(p, e):
        share = matmul(real_coupled[e], share_t[...]).astype(bf16)
        for way in range(2):
            for b in range(blocks):
                share_out[p][e, way, b] = share[b * size:(b + 1) * size, way * size:(way + 1) * size]
        for piece, rows in enumerate(pieces(p, e)):
            later_across(across(
                (part_ref(share_out[p].at[e, 0], rows), part_ref(share_out[p].at[e, 1], rows)),
                (part_ref(inbox.at[p, e, FROM_PREV], rows), part_ref(inbox.at[p, e, FROM_NEXT], rows)),
                inbox_landing(p, e, piece),
            ))

    def own_share_step(p, e):
        share_own[e] = matmul(real_coupled[e], own_t[...])

    def imag_mode_step(p, e, m):
        chosen = imag_source[p][e][slot[m]]
        coupled = matmul(matrices[m], side_by_side(*[chosen[c] for c in range(blocks)]))
        lower = (weight[m] * coupled).astype(bf16)
        upper = ((weight[m] + 1.0) * coupled).astype(bf16)
        for c in range(blocks):
            below[e, m, c] = lower[:, c * size:(c + 1) * size]
            above[e, m, c] = upper[:, c * size:(c + 1) * size]

    def imag_step(p, e):
        for m in range(MODES):
            imag_mode_step(p, e, m)

    def part_of(target):
        lower = [m for m in range(MODES) if 0 <= target - m - 1 < energies]
        upper = [m for m in range(MODES) if 0 <= target + m + 1 < energies]
        rows = []
        for b in range(blocks):
            terms = [below[target - m - 1, m, picks[m][b]] for m in lower]
            terms += [above[target + m + 1, m, picks[m][b]] for m in upper]
            rows.append(side_by_side(*terms))
        spans = [
            matrices_t[pl.ds(ms[0] * size, len(ms) * size), :] for ms in (lower, upper) if ms
        ]
        return matmul(on_top(*rows), on_top(*spans))

    def part_step(p, e, up):
        part = part_of(e + energies if up else e - energies).astype(bf16)
        source = part_out[p].at[1 if up else 0, e]
        for b in range(blocks):
            part_out[p][1 if up else 0, e, b] = part[b * size:(b + 1) * size]
        condition, send_part, place = (has_up, send_up, FROM_DOWN) if up else (has_down, send_down, FROM_UP)
        for piece, rows in enumerate(pieces(p, e)):
            later(condition, functools.partial(
                send_part, part_ref(source, rows), part_ref(inbox.at[p, e, place], rows), inbox_landing(p, e, piece)
            ))

    def own_part_step(p, e):
        part_own[e] = part_of(e)

    def close_step(p, e, piece=0):
        halved = e in HALVED[p]
        for b in [piece] if halved else range(blocks):
            rows = slice(b * size, (b + 1) * size)
            real = share_own[e, rows] + inbox[p, e, FROM_NEXT, b].astype(f32)
            real = (real + inbox[p, e, FROM_PREV, b].astype(f32)).astype(bf16)
            imag = part_own[e, rows] + inbox[p, e, FROM_DOWN, b].astype(f32)
            imag = (imag + inbox[p, e, FROM_UP, b].astype(f32)).astype(bf16)
            sigma = on_top(side_by_side(real, imag), side_by_side(-imag, real))
            both = wide_bare[e, b, pl.ds(0, size), :]
            product = matmul(both, sigma).astype(bf16)
            new = (both.astype(f32) + matmul(product, wide_bare[e, b])).astype(bf16)
            if p == passes - 1:
                out[0, 0, e, b] = new[:, :size]
                out[1, 0, e, b] = new[:, size:]
            else:
                real_current[p + 1][e][b] = new[:, :size]
                imag_source[p + 1][e][OWN, b] = new[:, size:]
        if p == passes - 1:
            return
        if halved:
            rows = pieces(p, e)[piece]
            later_across(imag_across(p + 1, e, rows))
            later(has_up, functools.partial(send_real_up, p + 1, e, rows))
            later(has_down, functools.partial(send_real_down, p + 1, e, rows))
            if piece == 0:
                closed.append(e)
            return
        closed.append(e)
        for condition, order, action in ((None, ACROSS, imag_across), (has_up, UPWARD, send_real_up), (has_down, DOWNWARD, send_real_down)):
            begin, end = in_turn(order[p + 1], closed[:-1]), in_turn(order[p + 1], closed)
            for turn in order[p + 1][begin:end]:
                if condition is None:
                    later_across(action(p + 1, turn))
                else:
                    later(condition, functools.partial(action, p + 1, turn))

    steps = {
        "Q": mode_step, "S": share_step, "O": own_share_step, "I": imag_step, "J": imag_mode_step,
        "U": functools.partial(part_step, up=True), "D": functools.partial(part_step, up=False),
        "A": own_part_step, "C": close_step,
    }
    waits = {"Q": rims_landed, "I": imag_landed, "J": imag_landed, "C": inbox_landed}
    def run(odd):
        nonlocal parity
        parity = odd
        waited.clear()
        for p in range(passes):
            closed.clear()
            for group in STEPS[odd][p]:
                calls = [(name[0], [int(digit) for digit in name[1:]]) for name in group.split("+")]
                for kind, at in calls:
                    if kind in waits:
                        waits[kind](p, *at)
                for kind, at in calls:
                    steps[kind](p, *at)
                send_all()

    parity = 0
    pl.when(is_even)(lambda: run(0))
    pl.when(is_odd)(lambda: run(1))

    everything = inbox.at[0]
    pltpu.make_async_copy(inbox, inbox, send_sem.at[0]).wait()
    pl.when(has_up)(lambda: pltpu.make_async_copy(everything, everything, send_sem.at[1]).wait())
    pl.when(has_down)(lambda: pltpu.make_async_copy(everything, everything, send_sem.at[2]).wait())


def shards(mom_count, en_count, green, bare, coupling, occupation, mode_shift, mode_offset, mode_block):
    _, _, energies, blocks, size, _ = green.shape
    assert energies == REACH and coupling.shape[0] == MODES and MODES == REACH
    pair = (blocks, size, size)
    vmem = pltpu.VMEM
    smem = pltpu.SMEM
    dma = pltpu.SemaphoreType.DMA
    scratch = [
        smem(occupation.shape, occupation.dtype),
        smem(mode_shift.shape, mode_shift.dtype),
        smem(mode_offset.shape, mode_offset.dtype),
        smem(mode_block.shape, mode_block.dtype),
        vmem(bare.shape, bf16),
        vmem(coupling.shape, bf16),
        vmem((MODES, size, size), bf16),
        vmem((MODES * size, size), bf16),
        vmem((MODES * size, 2 * size), bf16),
        vmem((MODES * size, size), bf16),
        vmem((energies, blocks, 2 * size, 2 * size), bf16),
        vmem((energies, blocks * size, MODES * size), bf16),
        vmem((energies, MODES) + pair, bf16),
        vmem((energies, MODES) + pair, bf16),
        vmem((energies, blocks * size, size), f32),
        vmem((energies, blocks * size, size), f32),
        [[vmem(pair, bf16) for _ in range(energies)] for _ in range(PASSES)],
        [[vmem(pair, bf16) for _ in range(energies)] for _ in range(PASSES)],
        [[vmem(pair, bf16) for _ in range(energies)] for _ in range(PASSES)],
        [[vmem((3,) + pair, bf16) for _ in range(energies)] for _ in range(PASSES)],
        [vmem((energies, 2) + pair, bf16) for _ in range(PASSES)],
        [vmem((2, energies) + pair, bf16) for _ in range(PASSES)],
        vmem((PASSES, energies, 4) + pair, bf16),
        dma((2, REACH + 1)),
        dma((REACH,)),
        dma((PASSES * energies + sum(map(len, HALVED)),)),
        dma((3,)),
        dma((6,)),
    ]
    whole = pl.BlockSpec(memory_space=pltpu.VMEM)
    anywhere = pl.BlockSpec(memory_space=pltpu.HBM)
    return pl.pallas_call(
        functools.partial(kernel, mom_count, en_count, PASSES),
        out_shape=jax.ShapeDtypeStruct(green.shape, green.dtype),
        in_specs=[anywhere] * 7,
        out_specs=whole,
        scratch_shapes=scratch,
        compiler_params=pltpu.CompilerParams(
            collective_id=0, has_side_effects=True, vmem_limit_bytes=40 * 1024 * 1024
        ),
        name="born_passes",
    )(*[pltpu.with_memory_space_constraint(a, pltpu.HBM) for a in (occupation, mode_shift, mode_offset, mode_block, green, bare, coupling)])


def solution(mesh):
    spread = P(None, "mom", "en", None, None, None)
    return jax.shard_map(
        functools.partial(shards, mesh.shape["mom"], mesh.shape["en"]),
        mesh=mesh,
        in_specs=(spread, spread, P(), P(), P(), P(), P()),
        out_specs=spread,
        check_vma=False,
    )
```
